32 devices in a mesh: track: 8 (over z, x), lane: 4 (over y, core).
Axes of the slice: x: 2, y: 2, z: 4, core: 2. Of those that a mesh axis runs over, the one named last changes fastest.
Arguments:
- signal: float32 [8, 4, 4096, 512], P('track', 'lane'), may hold values from -8 to 8, as said below
- tap_gain: float32 [3, 512], replicated, may hold values from 0.3 to 1.2
Outputs:
- filtered: float32 [8, 4, 4096, 512], P('track', 'lane')
The draws below stay inside these ranges and needn't reach their ends.
Inputs may be any that keep to these rules, and one draw needn't show every extreme that they name: signal holds numbers from -8 to 8.
All inputs are finite; a program needn't handle non-finite values.
Results may differ from the reference program's by a relative error of at most 0.0003.
Values sent between devices are 32-bit elements.
A program may use at most 64 MiB of HBM per device.

```python
import jax
import jax.numpy as jnp

STEPS_DEV = 4096
CHANNELS = 512
SEGMENTS = 8
RECORDS = 4


def draw_signal(key, part):
    keys = jax.random.split(key, 2)
    loud = jnp.exp(jax.random.uniform(keys[0], (SEGMENTS, RECORDS, 1, CHANNELS), jnp.float32, -1.2, 1.2))
    noise = jax.random.normal(keys[1], (SEGMENTS, RECORDS, STEPS_DEV, CHANNELS), jnp.float32)
    return jnp.clip(loud * noise, -8.0, 8.0)


def setup_inputs(seed: int = 0) -> dict:
    seeds = jax.random.split(jax.random.key(seed), 3)
    signal = draw_signal(jax.random.fold_in(seeds[2], 71), 0)
    tap_gain = jnp.clip(jax.random.uniform(seeds[1], (3, CHANNELS), jnp.float32, 0.3, 1.2), 0.3, 1.2)
    return {"signal": signal, "tap_gain": tap_gain}


def reference(signal, tap_gain):
    wide_in = signal.astype(jnp.float32)
    mixed = tap_gain[0] * wide_in + tap_gain[1] * jnp.roll(wide_in, 1, axis=0) + tap_gain[2] * jnp.roll(wide_in, 2, axis=0)
    filtered = jnp.tanh(mixed).astype(jnp.float32)
    return filtered
```

```python
import functools

import jax
import jax.numpy as jnp
from jax import lax
from jax.experimental import pallas as pl
from jax.experimental.pallas import tpu as pltpu
from jax.sharding import PartitionSpec as P

CHUNKS = 64
AHEAD = 6
BAND = 32


def kernel(n, chunks, signal, gain, out, own, far, near, local_sem, send_sem, far_sem, near_sem):
    me = lax.axis_index("track")
    odd = lax.rem(me, 2)
    partner = me + 1 - 2 * odd
    after, before = lax.rem(me + 2, n), lax.rem(me + n - 2, n)
    steps = signal.shape[0]
    rows = steps // chunks

    def part(ref, k):
        return ref.at[pl.ds(pl.multiple_of(k * rows, rows), rows)]

    def to_after(k):
        return pltpu.make_async_remote_copy(
            part(signal, k), part(far, k), send_sem.at[0], far_sem.at[k],
            device_id={"track": after}, device_id_type=pl.DeviceIdType.MESH)

    def to_partner(source, k):
        return pltpu.make_async_remote_copy(
            part(source, k), part(near, k), send_sem.at[1], near_sem.at[k],
            device_id={"track": partner}, device_id_type=pl.DeviceIdType.MESH)

    def send(k):
        to_after(k).start()

        @pl.when(odd == 0)
        def _():
            to_partner(signal, k).start()

    load = pltpu.make_async_copy(signal, own, local_sem)
    load.start()

    barrier = pltpu.get_barrier_semaphore()
    for other in (partner, after, before):
        pl.semaphore_signal(barrier, inc=1, device_id={"track": other}, device_id_type=pl.DeviceIdType.MESH)
    pl.semaphore_wait(barrier, 3)

    @pl.loop(0, min(AHEAD, chunks))
    def _(k):
        send(k)

    load.wait()

    def mix(k):
        to_partner(signal, k).wait_recv()


        @pl.loop(0, rows // BAND)
        def _(b):
            at = pl.ds(pl.multiple_of(k * rows + b * BAND, BAND), BAND)
            out[at] = jnp.tanh(gain[0:1] * own[at] + gain[1:2] * near[at] + gain[2:3] * far[at])

    @pl.loop(0, chunks)
    def _(k):
        to_after(k).wait_recv()

        @pl.when(odd == 1)
        def _():
            to_partner(far, k).start()

        @pl.when(k + AHEAD < chunks)
        def _():
            send(k + AHEAD)

        @pl.when(k > 0)
        def _():
            mix(k - 1)

    mix(chunks - 1)
    pltpu.make_async_remote_copy(
        signal, far, send_sem.at[0], far_sem.at[0],
        device_id={"track": after}, device_id_type=pl.DeviceIdType.MESH).wait_send()
    pltpu.make_async_remote_copy(
        signal, near, send_sem.at[1], near_sem.at[0],
        device_id={"track": partner}, device_id_type=pl.DeviceIdType.MESH).wait_send()


def solution(mesh):
    n = mesh.shape["track"]

    def local(signal, tap_gain):
        steps, channels = signal.shape[-2:]
        block = (steps, channels)
        out = pl.pallas_call(
            functools.partial(kernel, n, CHUNKS),
            out_shape=pltpu.VMEM(block, jnp.float32),
            in_specs=[pl.BlockSpec(memory_space=pltpu.HBM), pl.BlockSpec(memory_space=pltpu.VMEM)],
            out_specs=pl.BlockSpec(memory_space=pltpu.VMEM),
            scratch_shapes=[
                pltpu.VMEM(block, jnp.float32),
                pltpu.VMEM(block, jnp.float32),
                pltpu.VMEM(block, jnp.float32),
                pltpu.SemaphoreType.DMA,
                pltpu.SemaphoreType.DMA((2,)),
                pltpu.SemaphoreType.DMA((CHUNKS,)),
                pltpu.SemaphoreType.DMA((CHUNKS,)),
            ],
            compiler_params=pltpu.CompilerParams(
                collective_id=0, has_side_effects=True, vmem_limit_bytes=48 * 1024 * 1024),
        )(signal.reshape(block), tap_gain)
        return out.reshape(signal.shape)

    in_specs = (P("track", "lane", None, None), P())
    out_specs = P("track", "lane", None, None)
    return jax.shard_map(local, mesh=mesh, in_specs=in_specs, out_specs=out_specs, check_vma=False)
```

```python
import functools

import jax
import jax.numpy as jnp
from jax import lax
from jax.experimental import pallas as pl
from jax.experimental.pallas import tpu as pltpu
from jax.sharding import PartitionSpec as P

CHUNKS = 32
EARLY = 2
AHEAD = 4
BAND = 32
LOGICAL = pl.DeviceIdType.MESH


def kernel(n, signal, gain, out, own, far, near, blend, load_sem, send_sem, far_sem, near_sem):
    me = lax.axis_index("track")
    odd = lax.rem(me, 2)
    partner = me + 1 - 2 * odd
    after, before = lax.rem(me + 2, n), lax.rem(me + n - 2, n)
    rows = signal.shape[0] // CHUNKS
    relayed = CHUNKS - EARLY

    def span(k, count=1):
        start = k * rows if isinstance(k, int) else pl.multiple_of(k * rows, rows)
        return pl.ds(start, count * rows)

    def to_after(source, dest):
        return lambda k: pltpu.make_async_remote_copy(
            source, far.at[dest], send_sem.at[0], far_sem.at[k],
            device_id={"track": after}, device_id_type=LOGICAL)

    def to_partner(source, dest):
        return lambda k: pltpu.make_async_remote_copy(
            source, near.at[dest], send_sem.at[1], near_sem.at[k],
            device_id={"track": partner}, device_id_type=LOGICAL)

    def wait_far(k):
        to_after(own.at[span(k)], span(k))(k).wait_recv()

    def wait_near(k):
        to_partner(own.at[span(k)], span(k))(k).wait_recv()

    def send(k):
        plain = jnp.logical_or(odd == 1, k < relayed)

        @pl.when(plain)
        def _():
            to_after(own.at[span(k)], span(k))(k).start()

        @pl.when(jnp.logical_not(plain))
        def _():
            to_after(blend.at[span(k - relayed)], span(k))(k).start()

        @pl.when(odd == 0)
        def _():
            to_partner(own.at[span(k)], span(k))(k).start()

    def bands(k, body):
        @pl.loop(0, rows // BAND)
        def _(b):
            body(pl.ds(pl.multiple_of(k * rows + b * BAND, BAND), BAND))

    def mix(k):
        wait_near(k)

        def body(at):
            out[at] = jnp.tanh(gain[0:1] * own[at] + gain[1:2] * near[at] + gain[2:3] * far[at])

        bands(k, body)

    def mix_blended(k):
        def body(at):
            out[at] = jnp.tanh(gain[0:1] * own[at] + far[at])

        bands(k, body)

    head = pltpu.make_async_copy(signal.at[span(0, AHEAD)], own.at[span(0, AHEAD)], load_sem.at[0])
    rest = pltpu.make_async_copy(
        signal.at[span(AHEAD, CHUNKS - AHEAD)], own.at[span(AHEAD, CHUNKS - AHEAD)], load_sem.at[1])
    head.start()
    rest.start()

    barrier = pltpu.get_barrier_semaphore()
    for other in (partner, before):
        pl.semaphore_signal(barrier, inc=1, device_id={"track": other}, device_id_type=LOGICAL)
    pl.semaphore_wait(barrier, 2)

    @pl.when(odd == 1)
    def _():
        @pl.loop(relayed, CHUNKS)
        def _(k):
            to_partner(signal.at[span(k)], span(k))(k).start()

    head.wait()

    @pl.loop(0, AHEAD)
    def _(k):
        send(k)

    rest.wait()

    def step(k):
        wait_far(k)

        @pl.when(jnp.logical_and(odd == 1, k < relayed))
        def _():
            to_partner(far.at[span(k)], span(k))(k).start()

        @pl.when(k + AHEAD < CHUNKS)
        def _():
            send(k + AHEAD)

        @pl.when(jnp.logical_and(odd == 1, k > 0))
        def _():
            mix(k - 1)

        @pl.when(jnp.logical_and(odd == 0, k > relayed))
        def _():
            mix_blended(k - 1)

        @pl.when(jnp.logical_and(odd == 0, k >= EARLY))
        def _():
            mix(k - EARLY)

    pl.loop(0, CHUNKS // 2)(step)

    @pl.when(odd == 0)
    def _():
        @pl.loop(relayed, CHUNKS)
        def _(k):
            wait_near(k)

            @pl.loop(0, rows // BAND)
            def _(b):
                at = pl.ds(pl.multiple_of(k * rows + b * BAND, BAND), BAND)
                to = pl.ds(pl.multiple_of((k - relayed) * rows + b * BAND, BAND), BAND)
                blend[to] = gain[1:2] * near[at] + gain[2:3] * own[at]

    pl.loop(CHUNKS // 2, CHUNKS)(step)

    @pl.when(odd == 1)
    def _():
        mix(CHUNKS - 1)

    @pl.when(odd == 0)
    def _():
        mix_blended(CHUNKS - 1)

    to_after(own, span(0, CHUNKS))(0).wait_send()
    to_partner(own, span(0, CHUNKS))(0).wait_send()


def solution(mesh):
    n = mesh.shape["track"]

    def local(signal, tap_gain):
        steps, channels = signal.shape[-2:]
        block = (steps, channels)
        out = pl.pallas_call(
            functools.partial(kernel, n),
            out_shape=pltpu.VMEM(block, jnp.float32),
            in_specs=[pl.BlockSpec(memory_space=pltpu.HBM), pl.BlockSpec(memory_space=pltpu.VMEM)],
            out_specs=pl.BlockSpec(memory_space=pltpu.VMEM),
            scratch_shapes=[
                pltpu.VMEM(block, jnp.float32),
                pltpu.VMEM(block, jnp.float32),
                pltpu.VMEM(block, jnp.float32),
                pltpu.VMEM((steps // CHUNKS * EARLY, channels), jnp.float32),
                pltpu.SemaphoreType.DMA((2,)),
                pltpu.SemaphoreType.DMA((2,)),
                pltpu.SemaphoreType.DMA((CHUNKS,)),
                pltpu.SemaphoreType.DMA((CHUNKS,)),
            ],
            compiler_params=pltpu.CompilerParams(
                collective_id=0, has_side_effects=True, vmem_limit_bytes=48 * 1024 * 1024),
        )(signal.reshape(block), tap_gain)
        return out.reshape(signal.shape)

    in_specs = (P("track", "lane", None, None), P())
    out_specs = P("track", "lane", None, None)
    return jax.shard_map(local, mesh=mesh, in_specs=in_specs, out_specs=out_specs, check_vma=False)
```

```python
import functools

import jax
import jax.numpy as jnp
from jax import lax
from jax.experimental import pallas as pl
from jax.experimental.pallas import tpu as pltpu
from jax.sharding import PartitionSpec as P

CHUNKS = 32
EARLY = 2
AHEAD = 4
BAND = 32
TAIL = 4
LOGICAL = pl.DeviceIdType.MESH


def kernel(n, signal, gain, out, own, far, near, blend, load_sem, send_sem, far_sem, near_sem):
    me = lax.axis_index("track")
    odd = lax.rem(me, 2)
    partner = me + 1 - 2 * odd
    after, before = lax.rem(me + 2, n), lax.rem(me + n - 2, n)
    rows = signal.shape[0] // CHUNKS
    relayed = CHUNKS - EARLY
    last = CHUNKS - 1

    def span(k, count=1):
        start = k * rows if isinstance(k, int) else pl.multiple_of(k * rows, rows)
        return pl.ds(start, count * rows)

    def to_after(source, dest):
        return lambda k: pltpu.make_async_remote_copy(
            source, far.at[dest], send_sem.at[0], far_sem.at[k],
            device_id={"track": after}, device_id_type=LOGICAL)

    def to_partner(source, dest):
        return lambda k: pltpu.make_async_remote_copy(
            source, near.at[dest], send_sem.at[1], near_sem.at[k],
            device_id={"track": partner}, device_id_type=LOGICAL)

    def wait_far(k):
        to_after(own.at[span(k)], span(k))(k).wait_recv()

    def wait_near(k):
        to_partner(own.at[span(k)], span(k))(k).wait_recv()

    def send(k):
        plain = jnp.logical_or(odd == 1, k < relayed)

        @pl.when(plain)
        def _():
            to_after(own.at[span(k)], span(k))(k).start()

        @pl.when(jnp.logical_not(plain))
        def _():
            to_after(blend.at[span(k - relayed)], span(k))(k).start()

        @pl.when(odd == 0)
        def _():
            to_partner(own.at[span(k)], span(k))(k).start()

    def piece(j, base=last):
        return pl.ds(base * rows + j * (rows // TAIL), rows // TAIL)

    def send_tail():
        for j in range(TAIL):
            @pl.when(odd == 1)
            def _():
                to_after(own.at[piece(j)], piece(j))(last + j).start()

            @pl.when(odd == 0)
            def _():
                to_after(blend.at[piece(j, last - relayed)], piece(j))(last + j).start()
                to_partner(own.at[piece(j)], piece(j))(last + j).start()

    def band(at):
        out[at] = jnp.tanh(gain[0:1] * own[at] + gain[1:2] * near[at] + gain[2:3] * far[at])

    def band_blended(at):
        out[at] = jnp.tanh(gain[0:1] * own[at] + far[at])

    def bands(k, body):
        @pl.loop(0, rows // BAND)
        def _(b):
            body(pl.ds(pl.multiple_of(k * rows + b * BAND, BAND), BAND))

    def mix(k):
        wait_near(k)
        bands(k, band)

    def mix_blended(k):
        bands(k, band_blended)

    def mix_piece(j):
        to_after(own.at[piece(j)], piece(j))(last + j).wait_recv()

        @pl.when(odd == 1)
        def _():
            to_partner(own.at[piece(j)], piece(j))(last + j).wait_recv()
            band(piece(j))

        @pl.when(odd == 0)
        def _():
            band_blended(piece(j))

    head = pltpu.make_async_copy(signal.at[span(0)], own.at[span(0)], load_sem.at[0])
    rest = pltpu.make_async_copy(
        signal.at[span(1, CHUNKS - 1)], own.at[span(1, CHUNKS - 1)], load_sem.at[1])
    head.start()
    rest.start()

    barrier = pltpu.get_barrier_semaphore()
    for other in (partner, before):
        pl.semaphore_signal(barrier, inc=1, device_id={"track": other}, device_id_type=LOGICAL)
    pl.semaphore_wait(barrier, 2)

    @pl.when(odd == 1)
    def _():
        @pl.loop(relayed, CHUNKS)
        def _(k):
            to_partner(signal.at[span(k)], span(k))(k).start()

    head.wait()
    send(0)
    rest.wait()
    pl.loop(1, AHEAD)(send)

    def step(k):
        wait_far(k)

        @pl.when(jnp.logical_and(odd == 1, k < relayed))
        def _():
            to_partner(far.at[span(k)], span(k))(k).start()

        @pl.when(k + AHEAD < last)
        def _():
            send(k + AHEAD)

        @pl.when(k + AHEAD == last)
        def _():
            send_tail()

        @pl.when(jnp.logical_and(odd == 1, k > 0))
        def _():
            mix(k - 1)

        @pl.when(jnp.logical_and(odd == 0, k > relayed))
        def _():
            mix_blended(k - 1)

        @pl.when(jnp.logical_and(odd == 0, k >= EARLY))
        def _():
            mix(k - EARLY)

    pl.loop(0, CHUNKS // 2)(step)

    @pl.when(odd == 0)
    def _():
        @pl.loop(relayed, CHUNKS)
        def _(k):
            wait_near(k)

            @pl.loop(0, rows // BAND)
            def _(b):
                at = pl.ds(pl.multiple_of(k * rows + b * BAND, BAND), BAND)
                to = pl.ds(pl.multiple_of((k - relayed) * rows + b * BAND, BAND), BAND)
                blend[to] = gain[1:2] * near[at] + gain[2:3] * own[at]

    pl.loop(CHUNKS // 2, last)(step)

    @pl.when(odd == 1)
    def _():
        mix(last - 1)

    @pl.when(odd == 0)
    def _():
        mix_blended(last - 1)

    for j in range(TAIL - 1):
        mix_piece(j)

    @pl.when(odd == 0)
    def _():
        mix(relayed - 1)

    mix_piece(TAIL - 1)

    to_after(own, span(0, CHUNKS))(0).wait_send()
    to_partner(own, span(0, CHUNKS))(0).wait_send()


def solution(mesh):
    n = mesh.shape["track"]

    def local(signal, tap_gain):
        steps, channels = signal.shape[-2:]
        block = (steps, channels)
        out = pl.pallas_call(
            functools.partial(kernel, n),
            out_shape=pltpu.VMEM(block, jnp.float32),
            in_specs=[pl.BlockSpec(memory_space=pltpu.HBM), pl.BlockSpec(memory_space=pltpu.VMEM)],
            out_specs=pl.BlockSpec(memory_space=pltpu.VMEM),
            scratch_shapes=[
                pltpu.VMEM(block, jnp.float32),
                pltpu.VMEM(block, jnp.float32),
                pltpu.VMEM(block, jnp.float32),
                pltpu.VMEM((steps // CHUNKS * EARLY, channels), jnp.float32),
                pltpu.SemaphoreType.DMA((2,)),
                pltpu.SemaphoreType.DMA((2,)),
                pltpu.SemaphoreType.DMA((CHUNKS - 1 + TAIL,)),
                pltpu.SemaphoreType.DMA((CHUNKS - 1 + TAIL,)),
            ],
            compiler_params=pltpu.CompilerParams(
                collective_id=0, has_side_effects=True, vmem_limit_bytes=48 * 1024 * 1024),
        )(signal.reshape(block), tap_gain)
        return out.reshape(signal.shape)

    in_specs = (P("track", "lane", None, None), P())
    out_specs = P("track", "lane", None, None)
    return jax.shard_map(local, mesh=mesh, in_specs=in_specs, out_specs=out_specs, check_vma=False)
```
